256 devices in a mesh: wide: 16 (over y_hi, x, core), blk: 16 (over y_lo, z).
Axes of the slice: x: 4, y: 4 (y_hi: 2, y_lo: 2; y = y_hi * 2 + y_lo), z: 8, core: 2. Of those that a mesh axis runs over, the one named last changes fastest.
Arguments:
- features: bfloat16 [2048, 768], P('blk'), may hold values from -6 to 6
- weights: bfloat16 [262144, 768], P(('wide', 'blk')), may hold values from -0.21875 to 0.21875
- momentum: bfloat16 [262144, 768], P(('wide', 'blk')), may hold values from -48 to 48
- targets: bfloat16 [2048, 262144], P(None, ('wide', 'blk')), may hold values from 0 to 1
Outputs:
- new_weights: bfloat16 [262144, 768], P(('wide', 'blk'))
- new_momentum: bfloat16 [262144, 768], P(('wide', 'blk'))
- feature_grad: bfloat16 [2048, 768], P('blk', 'wide')
The draws below stay inside these ranges and needn't reach their ends.
All inputs are finite; a program needn't handle non-finite values.
Results may differ from the reference program's by a relative error of at most 0.009.
Values may be sent and summed in bfloat16 or wider, within the bound.
No kernel may reach another device: no remote copies, remote signals or barrier semaphores. Data moves between devices by JAX's collectives and lax.ppermute only.
A program may use at most 64 MiB of HBM per device.

```python
import math
import jax
import jax.numpy as jnp
from jax import lax

D = 768
LABELS = 262144
ROWS = 2048


def block_scale(rng, shape, split, low, largest):
    def one(axis_at, blocks):
        draws = jax.random.uniform(jax.random.fold_in(jax.random.fold_in(rng, 6), axis_at), (blocks,), jnp.float32, low / len(split), largest / len(split))
        return jnp.repeat(jnp.exp(draws), shape[axis_at] // blocks).reshape((-1,) + (1,) * (len(shape) - axis_at - 1))

    factor_of = one(*split[0])
    for cut in split[1:]:
        factor_of = factor_of * one(*cut)
    return factor_of


def gaussian(rng, extent, scale, bound, cuts=(), held_as=jnp.bfloat16):
    values = scale * jax.random.normal(rng, extent, jnp.float32)
    if cuts:
        values = values * block_scale(rng, extent, cuts, -0.22, 0.18)
    return jnp.clip(values, -bound, bound).astype(held_as)


def setup_inputs(seed: int = 0) -> dict:
    keys = jax.random.split(jax.random.key(seed), 5)
    features = gaussian(keys[0], (ROWS, D), 1.0, 6.0, ((0, 16),))
    weights = gaussian(keys[1], (LABELS, D), D ** -0.5, 0.21875, ((0, 256),))
    momentum = gaussian(keys[2], (LABELS, D), 8.0, 48.0, ((0, 256),))
    targets = jnp.clip(1.0 * jax.random.uniform(keys[3], (ROWS, LABELS), jnp.float32) ** block_scale(keys[3], (ROWS, LABELS), ((1, 256),), -0.2, 0.2), 0.0, 1.0).astype(jnp.bfloat16)
    return dict(features=features, weights=weights, momentum=momentum, targets=targets)


def reference(features, weights, momentum, targets):
    width = math.gcd(LABELS, 8192)
    nblocks = LABELS // width

    def one_block(totals, index):
        start = (index * width).astype(jnp.int32)
        weight_rows = lax.dynamic_slice_in_dim(weights, start, width, 0)
        moment_rows = lax.dynamic_slice_in_dim(momentum, start, width, 0)
        target_cols = lax.dynamic_slice_in_dim(targets, start, width, 1)
        scores = jnp.dot(features, weight_rows.T, preferred_element_type=jnp.float32)
        errors = (jax.nn.sigmoid(scores) - target_cols.astype(jnp.float32)).astype(jnp.bfloat16)
        grad = jnp.dot(errors.T, features, preferred_element_type=jnp.float32)
        moment_new = (0.9 * moment_rows.astype(jnp.float32) + grad).astype(jnp.bfloat16)
        weight_new = (weight_rows.astype(jnp.float32) - 0.002 * moment_new.astype(jnp.float32)).astype(jnp.bfloat16)
        totals = totals + jnp.dot(errors, weight_rows, preferred_element_type=jnp.float32)
        return totals, (weight_new, moment_new)

    totals, (weight_all, moment_all) = lax.scan(one_block, jnp.zeros((ROWS, D), jnp.float32), jnp.arange(nblocks, dtype=jnp.int32))
    return weight_all.reshape(LABELS, D), moment_all.reshape(LABELS, D), totals.astype(jnp.bfloat16)
```

```python
import jax
import jax.numpy as jnp
from jax import lax
from jax.sharding import Mesh, PartitionSpec as P


WIDE = ("yh", "x", "c")
BLK = ("yl", "z")
BF = jnp.bfloat16
F32 = jnp.float32


def from_behind(block, axis, distance):
    n = lax.axis_size(axis)
    return lax.ppermute(block, axis, [(i, (i + distance) % n) for i in range(n)])


def ring_gather(piece, axis):
    n = lax.axis_size(axis)
    me = lax.axis_index(axis)
    got = [piece] + [from_behind(piece, axis, d) for d in range(1, n)]
    return me, got


def in_order(me, got):
    n = len(got)
    out = jnp.zeros((n,) + got[0].shape, got[0].dtype)
    for d, block in enumerate(got):
        out = lax.dynamic_update_index_in_dim(out, block, (me - d) % n, 0)
    return out


def ring_scatter(chunks, axis):
    n = lax.axis_size(axis)
    me = lax.axis_index(axis)
    got = [
        from_behind(lax.dynamic_index_in_dim(chunks, (me + d) % n, 0, False), axis, d)
        for d in range(1, n)
    ]
    own = lax.dynamic_index_in_dim(chunks, me, 0, False)
    return own, got


def total(own, got):
    s = own.astype(F32)
    for g in got:
        s = s + g.astype(F32)
    return s


def spread(piece, axis):
    n = lax.axis_size(axis)
    return lax.all_to_all(jnp.broadcast_to(piece[None], (n,) + piece.shape), axis, 0, 0)


def shards(features, weights, momentum, targets):
    ix, ic, iyh = lax.axis_index("x"), lax.axis_index("c"), lax.axis_index("yh")
    half_a, half_b = features[:64], features[64:]
    piece_a = lax.dynamic_slice_in_dim(half_a, (ic * 4 + ix) * 8, 8, 0)
    piece_b = lax.dynamic_slice_in_dim(half_b, (ic * 2 + iyh) * 16, 16, 0)
    a1 = spread(piece_a, BLK).reshape(128, 768)
    b1 = spread(piece_b, "z").reshape(128, 768)
    me_a, got_a = ring_gather(a1, "x")
    me_b, got_b = ring_gather(b1, ("yh", "yl"))
    a2 = in_order(me_a, got_a)
    b2 = in_order(me_b, got_b)
    a3 = lax.all_gather(a2, "c", axis=0)
    b3 = lax.all_gather(b2, "c", axis=0)
    fa = a3.reshape(2, 4, 16, 8, 768).transpose(2, 0, 1, 3, 4).reshape(16, 1, 64, 768)
    fb = (
        b3.reshape(2, 2, 2, 8, 16, 768).transpose(2, 3, 0, 1, 4, 5).reshape(16, 1, 64, 768)
    )
    full = jnp.concatenate([fa, fb], axis=1).reshape(2048, 768)

    scores = lax.dot_general(full, weights, (((1,), (1,)), ((), ())), preferred_element_type=F32)
    errors = (jax.nn.sigmoid(scores) - targets.astype(F32)).astype(BF)
    back = lax.dot_general(
        weights, errors, (((0,), (1,)), ((), ())), preferred_element_type=F32
    ).astype(BF)
    back = back.reshape(8, 2, 48, 2048)
    mine = lax.dynamic_index_in_dim(back, ic, 1, False)
    theirs = lax.dynamic_index_in_dim(back, 1 - ic, 1, False)
    part = (mine.astype(F32) + from_behind(theirs, "c", 1).astype(F32)).astype(BF)
    part = part.reshape(2, 4, 48, 2048)
    ca = part[:, :, :24].transpose(1, 0, 2, 3)
    cb = part[:, :, 24:].reshape(2, 4, 24, 2, 1024).transpose(0, 3, 1, 2, 4)
    cb = cb.reshape(4, 4, 24, 1024)
    oa, ga = ring_scatter(ca, "x")
    ob, gb = ring_scatter(cb, ("yh", "yl"))
    sa = total(oa, ga).astype(BF)
    sb = total(ob, gb).astype(BF)
    sa = sa.reshape(2, 24, 16, 128).transpose(0, 2, 1, 3).reshape(32, 24, 128)
    sb = sb.reshape(4, 24, 8, 128).transpose(0, 2, 1, 3).reshape(32, 24, 128)
    ta = lax.all_to_all(sa, ("yh", "yl", "z"), 0, 0)
    tb = lax.all_to_all(sb, ("x", "z"), 0, 0)
    feature_grad = jnp.concatenate(
        [jnp.sum(ta.astype(F32), 0), jnp.sum(tb.astype(F32), 0)], axis=0
    ).T.astype(BF)

    weight_grad = lax.dot_general(
        errors, full, (((0,), (0,)), ((), ())), preferred_element_type=F32
    )
    new_momentum = (0.9 * momentum.astype(F32) + weight_grad).astype(BF)
    new_weights = (weights.astype(F32) - 0.002 * new_momentum.astype(F32)).astype(BF)
    return (new_weights, new_momentum, feature_grad)


def solution(mesh):
    fine = Mesh(mesh.devices.reshape(2, 4, 2, 2, 8), WIDE + BLK)
    both = WIDE + BLK
    return jax.shard_map(
        shards,
        mesh=fine,
        in_specs=(P(BLK, None), P(both, None), P(both, None), P(None, both)),
        out_specs=(P(both, None), P(both, None), P(BLK, WIDE)),
        check_vma=False,
    )
```

```python
import jax
import jax.numpy as jnp
from jax import lax
from jax.experimental import pallas as pl
from jax.experimental.pallas import tpu as pltpu
from jax.sharding import Mesh, PartitionSpec as P


WIDE = ("yh", "x", "c")
BLK = ("yl", "z")
PLANE = ("yh", "x", "yl")
BF = jnp.bfloat16
F32 = jnp.float32
VMEM = pltpu.VMEM


SHAPE = (2, 4, 2, 2, 8)


def device(yh, x, c, yl, z):
    return (((yh * 4 + x) * 2 + c) * 2 + yl) * 8 + z


def groups(x_core):
    out = []
    for c in range(2):
        for z in range(8):
            for n in range(4):
                if c == x_core:
                    out.append([device(n // 2, x, c, n % 2, z) for x in range(4)])
                else:
                    out.append([device(y // 2, n, c, y % 2, z) for y in range(4)])
    return out


SMALL, LARGE = groups(1), groups(0)


def exchanged(chunks, which):
    return lax.all_to_all(chunks, WIDE + BLK, 0, 0, axis_index_groups=which)


def swapped(block):
    return lax.ppermute(block, "c", [(0, 1), (1, 0)])


def spread(piece, axis):
    n = lax.axis_size(axis)
    return lax.all_to_all(jnp.broadcast_to(piece[None], (n,) + piece.shape), axis, 0, 0)


def pick(array, index, dim):
    return lax.dynamic_index_in_dim(array, index, dim, False)


def nt(a, b):
    return lax.dot_general(a, b, (((1,), (1,)), ((), ())), preferred_element_type=F32)


def fill_errors(f_ref, w_ref, t_ref, e_ref):
    rows = f_ref[...]
    for n in range(4):
        labels = slice(n * 256, (n + 1) * 256)
        scores = nt(rows, w_ref[labels, :])
        t = t_ref[:, 0, :, labels].reshape(512, 256).astype(F32)
        e_ref[:, labels] = ((0.5 * jnp.tanh(0.5 * scores) + 0.5) - t).astype(BF)


def errors_kernel(half_ref, f_ref, w_ref, wt_ref, t_ref, e_ref, theirs_ref):
    del half_ref
    fill_errors(f_ref, w_ref, t_ref, e_ref)
    theirs_ref[0] = nt(wt_ref[0], e_ref[...]).astype(BF)


def errors_of(half, rows, weights, wt, targets):
    whole = pl.BlockSpec(memory_space=VMEM)
    return pl.pallas_call(
        errors_kernel,
        grid_spec=pltpu.PrefetchScalarGridSpec(
            num_scalar_prefetch=1,
            grid=(2,),
            in_specs=[
                pl.BlockSpec((512, 768), lambda g, h: (g, 0)),
                whole,
                whole,
                pl.BlockSpec((8, 1, 64, 1024), lambda g, h: (g, h[0], 0, 0)),
            ],
            out_specs=[
                pl.BlockSpec((512, 1024), lambda g, h: (g, 0)),
                pl.BlockSpec((1, 384, 512), lambda g, h: (g, 0, 0)),
            ],
        ),
        out_shape=[
            jax.ShapeDtypeStruct((1024, 1024), BF),
            jax.ShapeDtypeStruct((2, 384, 512), BF),
        ],
        cost_estimate=pl.CostEstimate(
            flops=3 * 1024 * 1024 * 768, bytes_accessed=7 << 20, transcendentals=1 << 20
        ),
        compiler_params=pltpu.CompilerParams(vmem_limit_bytes=20 << 20),
        name="errors",
    )(half, rows, weights, wt, targets.reshape(16, 2, 64, 1024))


def mine_kernel(wt_ref, e1_ref, e2_ref, out_ref):
    for n, e_ref in enumerate((e1_ref, e2_ref)):
        for g in range(2):
            out_ref[n, g] = nt(wt_ref[1], e_ref[g * 512 : (g + 1) * 512, :])


def mine_of(wt, errors1, errors2):
    whole = pl.BlockSpec(memory_space=VMEM)
    return pl.pallas_call(
        mine_kernel,
        in_specs=[whole] * 3,
        out_specs=whole,
        out_shape=jax.ShapeDtypeStruct((2, 2, 384, 512), F32),
        cost_estimate=pl.CostEstimate(
            flops=2 * 1024 * 1024 * 768, bytes_accessed=8 << 20, transcendentals=0
        ),
        compiler_params=pltpu.CompilerParams(vmem_limit_bytes=8 << 20),
        name="mine",
    )(wt, errors1, errors2)


def join_kernel(core_ref, m_ref, g1_ref, g2_ref, out_ref):
    core = core_ref[0]
    for n, g_ref in enumerate((g2_ref, g1_ref)):
        for p in range(8):
            for yl in range(2):
                rows = slice(p * 48, (p + 1) * 48)
                out_ref[slot(core, p % 4, p // 4, yl), :, n * 512 : (n + 1) * 512] = (
                    m_ref[n, yl, rows, :] + g_ref[yl, rows, :].astype(F32)
                ).astype(BF)


def join(core, mine, got1, got2):
    whole = pl.BlockSpec(memory_space=VMEM)
    return pl.pallas_call(
        join_kernel,
        in_specs=[pl.BlockSpec(memory_space=pltpu.SMEM)] + [whole] * 3,
        out_specs=whole,
        out_shape=jax.ShapeDtypeStruct((16, 48, 1024), BF),
        cost_estimate=pl.CostEstimate(flops=1 << 20, bytes_accessed=6 << 20, transcendentals=0),
        compiler_params=pltpu.CompilerParams(vmem_limit_bytes=8 << 20),
        name="join",
    )(core, mine, got1, got2)


def plane_kernel(t_ref, out_ref):
    s = t_ref[0].astype(F32)
    for p in range(1, 4):
        s = s + t_ref[p].astype(F32)
    s = s.astype(BF)
    for z in range(8):
        out_ref[z] = jnp.concatenate(
            [s[:, z * 64 : (z + 1) * 64], s[:, 512 + z * 64 : 512 + (z + 1) * 64]], axis=1
        )


def plane_total(t):
    whole = pl.BlockSpec(memory_space=VMEM)
    return pl.pallas_call(
        plane_kernel,
        in_specs=[whole],
        out_specs=whole,
        out_shape=jax.ShapeDtypeStruct((8, 48, 128), BF),
        cost_estimate=pl.CostEstimate(flops=1 << 20, bytes_accessed=2 << 20, transcendentals=0),
        compiler_params=pltpu.CompilerParams(vmem_limit_bytes=8 << 20),
        name="plane_total",
    )(t)


def update_kernel(e1_ref, e2_ref, f1_ref, f2_ref, w_ref, m_ref, nw_ref, nm_ref):
    dims = (((0,), (0,)), ((), ()))
    grad = lax.dot_general(e1_ref[...], f1_ref[...], dims, preferred_element_type=F32)
    grad = grad + lax.dot_general(e2_ref[...], f2_ref[...], dims, preferred_element_type=F32)
    momentum = (0.9 * m_ref[...].astype(F32) + grad).astype(BF)
    nm_ref[...] = momentum
    nw_ref[...] = (w_ref[...].astype(F32) - 0.002 * momentum.astype(F32)).astype(BF)


def update(errors1, errors2, rows1, rows2, weights, momentum):
    whole = pl.BlockSpec((1024, 768), lambda n: (0, 0))
    labels = pl.BlockSpec((256, 768), lambda n: (n, 0))
    columns = pl.BlockSpec((1024, 256), lambda n: (0, n))
    return pl.pallas_call(
        update_kernel,
        grid=(4,),
        in_specs=[columns, columns, whole, whole, labels, labels],
        out_specs=[labels, labels],
        out_shape=[jax.ShapeDtypeStruct((1024, 768), BF)] * 2,
        cost_estimate=pl.CostEstimate(
            flops=4 * 1024 * 1024 * 768, bytes_accessed=12 << 20, transcendentals=0
        ),
        compiler_params=pltpu.CompilerParams(vmem_limit_bytes=60 << 20),
        name="update",
    )(errors1, errors2, rows1, rows2, weights, momentum)


def slot(core, x, yh, yl):
    y = yh * 2 + yl
    return jnp.where(core == 0, x * 4 + y, y * 4 + x)


def by_block_kernel(core_ref, in_ref, out_ref):
    core = core_ref[0]
    for yh in range(2):
        for x in range(4):
            for yl in range(2):
                out_ref[yl * 8 : (yl + 1) * 8, yh * 4 + x] = in_ref[slot(core, x, yh, yl)]


def by_block(core, rows):
    whole = pl.BlockSpec(memory_space=VMEM)
    out = pl.pallas_call(
        by_block_kernel,
        in_specs=[pl.BlockSpec(memory_space=pltpu.SMEM), whole],
        out_specs=whole,
        out_shape=jax.ShapeDtypeStruct((16, 8, 8, 768), BF),
        cost_estimate=pl.CostEstimate(flops=1 << 20, bytes_accessed=3 << 20, transcendentals=0),
        compiler_params=pltpu.CompilerParams(vmem_limit_bytes=8 << 20),
        name="by_block",
    )(core, rows.reshape(16, 8, 8, 768))
    return out.reshape(1024, 768)


def shards(features, weights, momentum, targets):
    ic = lax.axis_index("c")
    place = ic * 8 + lax.axis_index(("yh", "x"))
    piece = lax.dynamic_slice_in_dim(features, place * 8, 8, 0)
    a = spread(piece, "z")
    wt = weights.T.reshape(8, 2, 48, 1024)
    wt = jnp.stack(
        [pick(wt, 1 - ic, 1).reshape(384, 1024), pick(wt, ic, 1).reshape(384, 1024)]
    )
    a, wt = lax.optimization_barrier((a, wt))
    a = exchanged(jnp.broadcast_to(a.reshape(1, 64, 768), (4, 64, 768)), SMALL)
    a = exchanged(jnp.broadcast_to(a.reshape(1, 256, 768), (4, 256, 768)), LARGE)
    half = jnp.reshape(ic, (1,)).astype(jnp.int32)
    rows1 = by_block(half, a)
    rows2 = swapped(rows1)
    errors1, out1 = errors_of(half, rows1, weights, wt, targets)
    got1 = swapped(out1)
    errors2, out2 = errors_of(1 - half, rows2, weights, wt, targets)
    got2 = swapped(out2)
    part = join(half, mine_of(wt, errors1, errors2), got1, got2)
    t = exchanged(part.reshape(4, 4, 48, 1024), LARGE)
    t = exchanged(jnp.sum(t.astype(F32), 0).astype(BF), SMALL)
    t, errors1, errors2 = lax.optimization_barrier((t, errors1, errors2))
    u = lax.all_to_all(plane_total(t), "z", 0, 0)
    total = jnp.sum(u.astype(F32), 0).T.astype(BF)
    feature_grad = jnp.where(ic == 0, total, jnp.roll(total, 64, 0))
    new_weights, new_momentum = update(errors1, errors2, rows1, rows2, weights, momentum)
    return (new_weights, new_momentum, feature_grad)


def solution(mesh):
    fine = Mesh(mesh.devices.reshape(2, 4, 2, 2, 8), WIDE + BLK)
    both = WIDE + BLK
    return jax.shard_map(
        shards,
        mesh=fine,
        in_specs=(P(BLK, None), P(both, None), P(both, None), P(None, both)),
        out_specs=(P(both, None), P(both, None), P(BLK, WIDE)),
        check_vma=False,
    )
```

```python
import jax
import jax.numpy as jnp
from jax import lax
from jax.experimental import pallas as pl
from jax.experimental.pallas import tpu as pltpu
from jax.sharding import Mesh, PartitionSpec as P


WIDE = ("yh", "x", "c")
BLK = ("yl", "z")
BF = jnp.bfloat16
F32 = jnp.float32
VMEM = pltpu.VMEM
WHOLE = pl.BlockSpec(memory_space=VMEM)


def device(yh, x, c, yl, z):
    return (((yh * 4 + x) * 2 + c) * 2 + yl) * 8 + z


def plane_device(c, along, across, z):
    x, y = (across, along) if c == 0 else (along, across)
    return device(y // 2, x, c, y % 2, z)


LARGE = [
    [plane_device(c, n, m, z) for m in range(4)]
    for c in range(2)
    for n in range(4)
    for z in range(8)
]
SMALL = [
    [plane_device(c, n, m, z) for n in range(4) for z in range(8)]
    for c in range(2)
    for m in range(4)
]


def exchanged(chunks):
    return lax.all_to_all(chunks, WIDE + BLK, 0, 0, axis_index_groups=SMALL)


STEPS = (1, 3, 2)


def forward(block, step):
    route = [(g[i], g[(i + step) % 4]) for g in LARGE for i in range(4)]
    return lax.ppermute(block, WIDE + BLK, route)


def swapped(block):
    return lax.ppermute(block, "c", [(0, 1), (1, 0)])


def pick(array, index, dim):
    return lax.dynamic_index_in_dim(array, index, dim, False)


def nt(a, b):
    return lax.dot_general(a, b, (((1,), (1,)), ((), ())), preferred_element_type=F32)


def fill_errors(f_ref, w_ref, t_ref, e_ref):
    rows = f_ref[...]
    for n in range(4):
        labels = slice(n * 256, (n + 1) * 256)
        scores = nt(rows, w_ref[labels, :])
        t = t_ref[:, 0, :, labels].reshape(512, 256).astype(F32)
        e_ref[:, labels] = ((0.5 * jnp.tanh(0.5 * scores) + 0.5) - t).astype(BF)


def errors_kernel(half_ref, f_ref, w_ref, wt_ref, t_ref, e_ref, theirs_ref):
    del half_ref
    fill_errors(f_ref, w_ref, t_ref, e_ref)
    theirs_ref[0] = nt(wt_ref[0], e_ref[...]).astype(BF)


def errors_of(half, rows, weights, wt, targets):
    whole = pl.BlockSpec(memory_space=VMEM)
    return pl.pallas_call(
        errors_kernel,
        grid_spec=pltpu.PrefetchScalarGridSpec(
            num_scalar_prefetch=1,
            grid=(2,),
            in_specs=[
                pl.BlockSpec((512, 768), lambda g, h: (g, 0)),
                whole,
                whole,
                pl.BlockSpec((8, 1, 64, 1024), lambda g, h: (g, h[0], 0, 0)),
            ],
            out_specs=[
                pl.BlockSpec((512, 1024), lambda g, h: (g, 0)),
                pl.BlockSpec((1, 384, 512), lambda g, h: (g, 0, 0)),
            ],
        ),
        out_shape=[
            jax.ShapeDtypeStruct((1024, 1024), BF),
            jax.ShapeDtypeStruct((2, 384, 512), BF),
        ],
        cost_estimate=pl.CostEstimate(
            flops=3 * 1024 * 1024 * 768, bytes_accessed=7 << 20, transcendentals=1 << 20
        ),
        compiler_params=pltpu.CompilerParams(vmem_limit_bytes=20 << 20),
        name="errors",
    )(half, rows, weights, wt, targets.reshape(16, 2, 64, 1024))


def mine_kernel(wt_ref, e1_ref, e2_ref, out_ref):
    for n, e_ref in enumerate((e1_ref, e2_ref)):
        for g in range(2):
            out_ref[n, g] = nt(wt_ref[1], e_ref[g * 512 : (g + 1) * 512, :])


def mine_of(wt, errors1, errors2):
    whole = pl.BlockSpec(memory_space=VMEM)
    return pl.pallas_call(
        mine_kernel,
        in_specs=[whole] * 3,
        out_specs=whole,
        out_shape=jax.ShapeDtypeStruct((2, 2, 384, 512), F32),
        cost_estimate=pl.CostEstimate(
            flops=2 * 1024 * 1024 * 768, bytes_accessed=8 << 20, transcendentals=0
        ),
        compiler_params=pltpu.CompilerParams(vmem_limit_bytes=8 << 20),
        name="mine",
    )(wt, errors1, errors2)


def join_kernel(at_ref, m_ref, g1_ref, g2_ref, *out_refs):
    core, x, y = at_ref[0], at_ref[1], at_ref[2]
    for step, out_ref in zip((0,) + STEPS, out_refs):
        for r in range(4):
            to_x = jnp.where(core == 0, (x + step) % 4, r)
            to_y = jnp.where(core == 0, r, (y + step) % 4)
            p, yl = (to_y // 2) * 4 + to_x, to_y % 2
            for n, g_ref in enumerate((g2_ref, g1_ref)):
                out_ref[r, :, n * 512 : (n + 1) * 512] = (
                    m_ref[n, yl, p] + g_ref[yl, p].astype(F32)
                ).astype(BF)


def join(at, mine, got1, got2):
    return pl.pallas_call(
        join_kernel,
        in_specs=[pl.BlockSpec(memory_space=pltpu.SMEM)] + [WHOLE] * 3,
        out_specs=[WHOLE] * 4,
        out_shape=[jax.ShapeDtypeStruct((4, 48, 1024), BF)] * 4,
        cost_estimate=pl.CostEstimate(flops=1 << 20, bytes_accessed=6 << 20, transcendentals=0),
        compiler_params=pltpu.CompilerParams(vmem_limit_bytes=8 << 20),
        name="join",
    )(
        at,
        mine.reshape(2, 2, 8, 48, 512),
        got1.reshape(2, 8, 48, 512),
        got2.reshape(2, 8, 48, 512),
    )


def large_kernel(*refs):
    out_ref = refs[4]
    for r in range(4):
        s = refs[0][r].astype(F32)
        for ref in refs[1:4]:
            s = s + ref[r].astype(F32)
        s = s.astype(BF)
        for z in range(8):
            out_ref[r * 8 + z] = jnp.concatenate(
                [s[:, z * 64 : (z + 1) * 64], s[:, 512 + z * 64 : 512 + (z + 1) * 64]], axis=1
            )


def large_total(*blocks):
    return pl.pallas_call(
        large_kernel,
        in_specs=[WHOLE] * 4,
        out_specs=WHOLE,
        out_shape=jax.ShapeDtypeStruct((32, 48, 128), BF),
        cost_estimate=pl.CostEstimate(flops=1 << 20, bytes_accessed=2 << 20, transcendentals=0),
        compiler_params=pltpu.CompilerParams(vmem_limit_bytes=8 << 20),
        name="large_total",
    )(*blocks)


def update_kernel(e1_ref, e2_ref, f1_ref, f2_ref, w_ref, m_ref, nw_ref, nm_ref):
    dims = (((0,), (0,)), ((), ()))
    grad = lax.dot_general(e1_ref[...], f1_ref[...], dims, preferred_element_type=F32)
    grad = grad + lax.dot_general(e2_ref[...], f2_ref[...], dims, preferred_element_type=F32)
    momentum = (0.9 * m_ref[...].astype(F32) + grad).astype(BF)
    nm_ref[...] = momentum
    nw_ref[...] = (w_ref[...].astype(F32) - 0.002 * momentum.astype(F32)).astype(BF)


def update(*operands):
    rows = pl.BlockSpec((1024, 768), lambda n: (0, 0))
    labels = pl.BlockSpec((256, 768), lambda n: (n, 0))
    columns = pl.BlockSpec((1024, 256), lambda n: (0, n))
    return pl.pallas_call(
        update_kernel,
        grid=(4,),
        in_specs=[columns, columns, rows, rows, labels, labels],
        out_specs=[labels, labels],
        out_shape=[jax.ShapeDtypeStruct((1024, 768), BF)] * 2,
        cost_estimate=pl.CostEstimate(
            flops=4 * 1024 * 1024 * 768, bytes_accessed=12 << 20, transcendentals=0
        ),
        compiler_params=pltpu.CompilerParams(vmem_limit_bytes=60 << 20),
        name="update",
    )(*operands)


def by_block_kernel(at_ref, *refs):
    core, x, y = at_ref[0], at_ref[1], at_ref[2]
    out_ref = refs[4]
    for step, in_ref in zip((0,) + STEPS, refs):
        for n in range(4):
            from_x = jnp.where(core == 0, (x - step) % 4, n)
            from_y = jnp.where(core == 0, n, (y - step) % 4)
            out_ref[from_y % 2, :, (from_y // 2) * 4 + from_x] = in_ref[n]


def by_block(at, blocks):
    out = pl.pallas_call(
        by_block_kernel,
        in_specs=[pl.BlockSpec(memory_space=pltpu.SMEM)] + [WHOLE] * 4,
        out_specs=WHOLE,
        out_shape=jax.ShapeDtypeStruct((2, 8, 8, 8, 768), BF),
        cost_estimate=pl.CostEstimate(flops=1 << 20, bytes_accessed=3 << 20, transcendentals=0),
        compiler_params=pltpu.CompilerParams(vmem_limit_bytes=8 << 20),
        name="by_block",
    )(at, *[block.reshape(4, 8, 8, 768) for block in blocks])
    return out.reshape(1024, 768)


def shards(features, weights, momentum, targets):
    ic = lax.axis_index("c")
    place = ic * 8 + lax.axis_index(("yh", "x"))
    piece = lax.dynamic_slice_in_dim(features, place * 8, 8, 0)
    a = exchanged(jnp.broadcast_to(piece[None], (32, 8, 768)))
    a, weights = lax.optimization_barrier((a, weights))
    a = a.reshape(256, 768)
    blocks = [a] + [forward(a, d) for d in STEPS]
    wt = weights.T.reshape(8, 2, 48, 1024)
    wt = jnp.stack(
        [pick(wt, 1 - ic, 1).reshape(384, 1024), pick(wt, ic, 1).reshape(384, 1024)]
    )
    blocks, wt = lax.optimization_barrier((blocks, wt))
    at = jnp.stack([ic, lax.axis_index("x"), lax.axis_index(("yh", "yl"))]).astype(jnp.int32)
    rows1 = by_block(at, blocks)
    rows2 = swapped(rows1)
    errors1, out1 = errors_of(at, rows1, weights, wt, targets)
    got1 = swapped(out1)
    errors2, out2 = errors_of(1 - at[:1], rows2, weights, wt, targets)
    got2 = swapped(out2)
    own, *chunks = join(at, mine_of(wt, errors1, errors2), got1, got2)
    got = [forward(chunk, d) for chunk, d in zip(chunks, STEPS)]
    s, errors1, errors2 = lax.optimization_barrier((large_total(own, *got), errors1, errors2))
    u = exchanged(s)
    new_weights, new_momentum = update(errors1, errors2, rows1, rows2, weights, momentum)
    total = jnp.sum(u.astype(F32), 0).T.astype(BF)
    feature_grad = jnp.where(ic == 0, total, jnp.roll(total, 64, 0))
    return (new_weights, new_momentum, feature_grad)


def solution(mesh):
    fine = Mesh(mesh.devices.reshape(2, 4, 2, 2, 8), WIDE + BLK)
    both = WIDE + BLK
    return jax.shard_map(
        shards,
        mesh=fine,
        in_specs=(P(BLK, None), P(both, None), P(both, None), P(None, both)),
        out_specs=(P(both, None), P(both, None), P(BLK, WIDE)),
        check_vma=False,
    )
```

```python
import functools

import jax
import jax.numpy as jnp
from jax import lax
from jax.experimental import pallas as pl
from jax.experimental.pallas import tpu as pltpu
from jax.sharding import Mesh, PartitionSpec as P


WIDE = ("yh", "x", "c")
BLK = ("yl", "z")
BF = jnp.bfloat16
F32 = jnp.float32
VMEM = pltpu.VMEM
WHOLE = pl.BlockSpec(memory_space=VMEM)


def device(yh, x, c, yl, z):
    return (((yh * 4 + x) * 2 + c) * 2 + yl) * 8 + z


def plane_device(c, along, across, z):
    x, y = (across, along) if c == 0 else (along, across)
    return device(y // 2, x, c, y % 2, z)


LARGE = [
    [plane_device(c, n, m, z) for m in range(4)]
    for c in range(2)
    for n in range(4)
    for z in range(8)
]
SMALL = [
    [plane_device(c, n, m, z) for n in range(4) for z in range(8)]
    for c in range(2)
    for m in range(4)
]


GATHER = [
    [device(yh, x, 0, yl, z) for yl in range(2) for z in range(8)]
    for yh in range(2)
    for x in range(4)
] + [
    [device(yh, 2 * pair + n, 1, yl, z) for n in range(2) for z in range(8)]
    for yh in range(2)
    for yl in range(2)
    for pair in range(2)
]


def exchanged(chunks, which):
    return lax.all_to_all(chunks, WIDE + BLK, 0, 0, axis_index_groups=which)


STEPS = (1, 3, 2)


def forward(block, step):
    route = [(g[i], g[(i + step) % 4]) for g in LARGE for i in range(4)]
    return lax.ppermute(block, WIDE + BLK, route)


def swapped(block):
    return lax.ppermute(block, "c", [(0, 1), (1, 0)])


def nt(a, b):
    return lax.dot_general(a, b, (((1,), (1,)), ((), ())), preferred_element_type=F32)


def errors_kernel(step, at_ref, f1_ref, f2_ref, w_ref, t_ref, *refs):
    core, x, y = at_ref[0], at_ref[1], at_ref[2]
    rows = jnp.concatenate([f1_ref[...].reshape(256, 768), f2_ref[...].reshape(256, 768)])
    parts = [
        (half, place(half, x, y, step, n), e_ref)
        for half, e_ref in ((core, refs[-2]), (1 - core, refs[-1]))
        for n in range(2)
    ]
    span = [slice(m * 256, (m + 1) * 256) for m in range(4)]
    scores = nt(rows, w_ref[span[0], :])
    for m, labels in enumerate(span):
        following = nt(rows, w_ref[span[m + 1], :]) if m < 3 else None
        raised = 0.5 * jnp.tanh(0.5 * scores) + 0.5
        for n, (half, (yl, part), e_ref) in enumerate(parts):
            t = t_ref[yl, :, half, part, :, labels].reshape(128, 256).astype(F32)
            errors = (raised[n * 128 : (n + 1) * 128] - t).astype(BF)
            e_ref[yl, :, part, :, labels] = errors.reshape(8, 16, 256)
        scores = following


def errors_of(at, step, blocks, weights, targets, before):
    return pl.pallas_call(
        functools.partial(errors_kernel, step),
        in_specs=[pl.BlockSpec(memory_space=pltpu.SMEM)] + [WHOLE] * (4 + len(before)),
        out_specs=[WHOLE] * 2,
        out_shape=[jax.ShapeDtypeStruct((2, 8, 4, 16, 1024), BF)] * 2,
        input_output_aliases={5: 0, 6: 1} if before else {},
        cost_estimate=pl.CostEstimate(
            flops=1024 * 1024 * 768, bytes_accessed=5 << 20, transcendentals=1 << 19
        ),
        compiler_params=pltpu.CompilerParams(vmem_limit_bytes=12 << 20),
        name="errors",
    )(
        at,
        *[block.reshape(2, 8, 16, 768) for block in blocks],
        weights,
        targets.reshape(2, 8, 2, 4, 16, 1024),
        *before,
    )


def turned_kernel(at_ref, w_ref, out_ref, held_ref, sems):
    pieces = [pl.ds(m * 256, 256) for m in range(4)]
    copies = [
        pltpu.make_async_copy(w_ref.at[piece], held_ref.at[piece], sems.at[m])
        for m, piece in enumerate(pieces)
    ]
    for copy in copies:
        copy.start()
    for piece, copy in zip(pieces, copies):
        copy.wait()
        columns = held_ref[piece, :].T
        for core in range(2):
            mine = jnp.where(at_ref[0] == core, 1, 0)
            for p in range(8):
                first = (2 * p + core) * 48
                out_ref[mine, p * 48 : (p + 1) * 48, piece] = columns[first : first + 48, :]


def turned(at, weights):
    return pl.pallas_call(
        turned_kernel,
        in_specs=[
            pl.BlockSpec(memory_space=pltpu.SMEM),
            pl.BlockSpec(memory_space=pltpu.HBM),
        ],
        out_specs=[WHOLE] * 2,
        out_shape=[
            jax.ShapeDtypeStruct((2, 384, 1024), BF),
            jax.ShapeDtypeStruct((1024, 768), BF),
        ],
        scratch_shapes=[pltpu.SemaphoreType.DMA((4,))],
        cost_estimate=pl.CostEstimate(
            flops=1024 * 1024 * 768, bytes_accessed=5 << 20, transcendentals=0
        ),
        compiler_params=pltpu.CompilerParams(vmem_limit_bytes=8 << 20),
        name="turned",
    )(at, weights)


def theirs_kernel(wt_ref, e_ref, out_ref):
    for g in range(2):
        out_ref[g] = nt(wt_ref[0], e_ref[g * 512 : (g + 1) * 512, :]).astype(BF)


def theirs_of(wt, errors):
    return pl.pallas_call(
        theirs_kernel,
        in_specs=[WHOLE] * 2,
        out_specs=WHOLE,
        out_shape=jax.ShapeDtypeStruct((2, 384, 512), BF),
        cost_estimate=pl.CostEstimate(
            flops=1024 * 1024 * 768, bytes_accessed=4 << 20, transcendentals=0
        ),
        compiler_params=pltpu.CompilerParams(vmem_limit_bytes=8 << 20),
        name="theirs",
    )(wt, errors)


def mine_kernel(wt_ref, e1_ref, e2_ref, out_ref):
    for n, e_ref in enumerate((e1_ref, e2_ref)):
        for g in range(2):
            out_ref[n, g] = nt(wt_ref[1], e_ref[g * 512 : (g + 1) * 512, :])


def mine_of(wt, errors1, errors2):
    whole = pl.BlockSpec(memory_space=VMEM)
    return pl.pallas_call(
        mine_kernel,
        in_specs=[whole] * 3,
        out_specs=whole,
        out_shape=jax.ShapeDtypeStruct((2, 2, 384, 512), F32),
        cost_estimate=pl.CostEstimate(
            flops=2 * 1024 * 1024 * 768, bytes_accessed=8 << 20, transcendentals=0
        ),
        compiler_params=pltpu.CompilerParams(vmem_limit_bytes=8 << 20),
        name="mine",
    )(wt, errors1, errors2)


def join_kernel(at_ref, m_ref, g1_ref, g2_ref, *out_refs):
    core, x, y = at_ref[0], at_ref[1], at_ref[2]
    for step, out_ref in zip((0,) + STEPS, out_refs):
        for r in range(4):
            to_x = jnp.where(core == 0, (x + step) % 4, r)
            to_y = jnp.where(core == 0, r, (y + step) % 4)
            p, yl = (to_y // 2) * 4 + to_x, to_y % 2
            for n, g_ref in enumerate((g2_ref, g1_ref)):
                out_ref[r, :, n * 512 : (n + 1) * 512] = (
                    m_ref[n, yl, p] + g_ref[yl, p].astype(F32)
                ).astype(BF)


def join(at, mine, got1, got2):
    return pl.pallas_call(
        join_kernel,
        in_specs=[pl.BlockSpec(memory_space=pltpu.SMEM)] + [WHOLE] * 3,
        out_specs=[WHOLE] * 4,
        out_shape=[jax.ShapeDtypeStruct((4, 48, 1024), BF)] * 4,
        cost_estimate=pl.CostEstimate(flops=1 << 20, bytes_accessed=6 << 20, transcendentals=0),
        compiler_params=pltpu.CompilerParams(vmem_limit_bytes=8 << 20),
        name="join",
    )(
        at,
        mine.reshape(2, 2, 8, 48, 512),
        got1.reshape(2, 8, 48, 512),
        got2.reshape(2, 8, 48, 512),
    )


def large_kernel(*refs):
    out_ref = refs[4]
    for r in range(4):
        s = refs[0][r].astype(F32)
        for ref in refs[1:4]:
            s = s + ref[r].astype(F32)
        s = s.astype(BF)
        for z in range(8):
            out_ref[r * 8 + z] = jnp.concatenate(
                [s[:, z * 64 : (z + 1) * 64], s[:, 512 + z * 64 : 512 + (z + 1) * 64]], axis=1
            )


def large_total(*blocks):
    return pl.pallas_call(
        large_kernel,
        in_specs=[WHOLE] * 4,
        out_specs=WHOLE,
        out_shape=jax.ShapeDtypeStruct((32, 48, 128), BF),
        cost_estimate=pl.CostEstimate(flops=1 << 20, bytes_accessed=2 << 20, transcendentals=0),
        compiler_params=pltpu.CompilerParams(vmem_limit_bytes=8 << 20),
        name="large_total",
    )(*blocks)


def update_kernel(e1_ref, e2_ref, f1_ref, f2_ref, w_ref, m_ref, nw_ref, nm_ref):
    dims = (((0,), (0,)), ((), ()))
    grad = lax.dot_general(e1_ref[...], f1_ref[...], dims, preferred_element_type=F32)
    grad = grad + lax.dot_general(e2_ref[...], f2_ref[...], dims, preferred_element_type=F32)
    momentum = (0.9 * m_ref[...].astype(F32) + grad).astype(BF)
    nm_ref[...] = momentum
    nw_ref[...] = (w_ref[...].astype(F32) - 0.002 * momentum.astype(F32)).astype(BF)


def update(*operands):
    labels = pl.BlockSpec((256, 768), lambda n: (n, 0))
    columns = pl.BlockSpec((1024, 256), lambda n: (0, n))
    return pl.pallas_call(
        update_kernel,
        grid=(4,),
        in_specs=[columns, columns, WHOLE, WHOLE, labels, labels],
        out_specs=[labels, labels],
        out_shape=[jax.ShapeDtypeStruct((1024, 768), BF)] * 2,
        cost_estimate=pl.CostEstimate(
            flops=4 * 1024 * 1024 * 768, bytes_accessed=12 << 20, transcendentals=0
        ),
        compiler_params=pltpu.CompilerParams(vmem_limit_bytes=24 << 20),
        name="update",
    )(*operands)


def place(core, x, y, step, n):
    from_x, from_y = (x - step) % 4, (y - step) % 4
    return (
        jnp.where(core == 0, n, from_y % 2),
        jnp.where(core == 0, from_x, (from_y // 2) * 2 + n),
    )


def by_block_kernel(at_ref, *refs):
    out_ref = refs[4]
    for step, in_ref in zip((0,) + STEPS, refs):
        for n in range(2):
            yl, part = place(at_ref[0], at_ref[1], at_ref[2], step, n)
            out_ref[yl, :, part] = in_ref[n]


def by_block(at, blocks):
    out = pl.pallas_call(
        by_block_kernel,
        in_specs=[pl.BlockSpec(memory_space=pltpu.SMEM)] + [WHOLE] * 4,
        out_specs=WHOLE,
        out_shape=jax.ShapeDtypeStruct((2, 8, 4, 16, 768), BF),
        cost_estimate=pl.CostEstimate(flops=1 << 20, bytes_accessed=3 << 20, transcendentals=0),
        compiler_params=pltpu.CompilerParams(vmem_limit_bytes=8 << 20),
        name="by_block",
    )(at, *[block.reshape(2, 8, 16, 768) for block in blocks])
    return out.reshape(1024, 768)


def program(features, weights, momentum, targets):
    ic = lax.axis_index("c")
    ix, iyh, iyl = lax.axis_index("x"), lax.axis_index("yh"), lax.axis_index("yl")
    at = jnp.stack([ic, ix, iyh * 2 + iyl]).astype(jnp.int32)
    quarter = jnp.where(ic == 0, ix, iyh * 2 + ix % 2)
    piece = lax.dynamic_slice_in_dim(features, ic * 64 + quarter * 16, 16, 0)
    other = jnp.stack([1 - ic, ix, iyh * 2 + iyl]).astype(jnp.int32)
    piece, at, other = lax.optimization_barrier((piece, at, other))
    a = exchanged(jnp.broadcast_to(piece[None], (16, 16, 768)), GATHER)
    a, weights = lax.optimization_barrier((a, weights))
    a = a.reshape(256, 768)
    blocks = [a] + [forward(a, d) for d in STEPS]
    wt, held = turned(at, weights)
    errors, others = (), []
    for step, block in zip((0,) + STEPS, blocks):
        if step == 1:
            block, errors, wt = lax.optimization_barrier((block, errors, wt))
        others.append(swapped(block))
        errors = errors_of(at, step, (block, others[-1]), held, targets, errors)
    errors1, errors2 = (e.reshape(1024, 1024) for e in errors)
    got1 = swapped(theirs_of(wt, errors1))
    got2 = swapped(theirs_of(wt, errors2))
    own, *chunks = join(at, mine_of(wt, errors1, errors2), got1, got2)
    got = [forward(chunk, d) for chunk, d in zip(chunks, STEPS)]
    rows1, rows2 = by_block(at, blocks), by_block(other, others)
    updated = update(errors1, errors2, rows1, rows2, held, momentum)
    got, updated = lax.optimization_barrier((got, updated))
    new_weights, new_momentum = updated
    u = exchanged(large_total(own, *got), SMALL)
    total = jnp.sum(u.astype(F32), 0).T.astype(BF)
    feature_grad = jnp.where(ic == 0, total, jnp.roll(total, 64, 0))
    return (new_weights, new_momentum, feature_grad)


def solution(mesh):
    fine = Mesh(mesh.devices.reshape(2, 4, 2, 2, 8), WIDE + BLK)
    both = WIDE + BLK
    return jax.shard_map(
        program,
        mesh=fine,
        in_specs=(P(BLK, None), P(both, None), P(both, None), P(None, both)),
        out_specs=(P(both, None), P(both, None), P(BLK, WIDE)),
        check_vma=False,
    )
```

```python
import functools

import jax
import jax.numpy as jnp
from jax import lax
from jax.experimental import pallas as pl
from jax.experimental.pallas import tpu as pltpu
from jax.sharding import Mesh, PartitionSpec as P


WIDE = ("yh", "x", "c")
BLK = ("yl", "z")
BF = jnp.bfloat16
F32 = jnp.float32
VMEM = pltpu.VMEM
WHOLE = pl.BlockSpec(memory_space=VMEM)


def device(yh, x, c, yl, z):
    return (((yh * 4 + x) * 2 + c) * 2 + yl) * 8 + z


def plane_device(c, along, across, z):
    x, y = (across, along) if c == 0 else (along, across)
    return device(y // 2, x, c, y % 2, z)


LARGE = [
    [plane_device(c, n, m, z) for m in range(4)]
    for c in range(2)
    for n in range(4)
    for z in range(8)
]
SMALL = [
    [plane_device(c, n, m, z) for n in range(4) for z in range(8)]
    for c in range(2)
    for m in range(4)
]


GATHER = [
    [device(yh, x, 0, yl, z) for yl in range(2) for z in range(8)]
    for yh in range(2)
    for x in range(4)
] + [
    [device(yh, 2 * pair + n, 1, yl, z) for n in range(2) for z in range(8)]
    for yh in range(2)
    for yl in range(2)
    for pair in range(2)
]


def exchanged(chunks, which):
    return lax.all_to_all(chunks, WIDE + BLK, 0, 0, axis_index_groups=which)


STEPS = (1, 3, 2)


def forward(block, step):
    route = [(g[i], g[(i + step) % 4]) for g in LARGE for i in range(4)]
    return lax.ppermute(block, WIDE + BLK, route)


def swapped(block):
    return lax.ppermute(block, "c", [(0, 1), (1, 0)])


def nt(a, b):
    return lax.dot_general(a, b, (((1,), (1,)), ((), ())), preferred_element_type=F32)


def errors_kernel(step, at_ref, f1_ref, f2_ref, w_ref, t_ref, *refs):
    core, x, y = at_ref[0], at_ref[1], at_ref[2]
    rows = jnp.concatenate([f1_ref[...].reshape(256, 768), f2_ref[...].reshape(256, 768)])
    parts = [
        (half, place(half, x, y, step, n), e_ref)
        for half, e_ref in ((core, refs[-2]), (1 - core, refs[-1]))
        for n in range(2)
    ]
    span = [slice(m * 256, (m + 1) * 256) for m in range(4)]
    scores = nt(rows, w_ref[span[0], :])
    for m, labels in enumerate(span):
        following = nt(rows, w_ref[span[m + 1], :]) if m < 3 else None
        raised = 0.5 * jnp.tanh(0.5 * scores) + 0.5
        for n, (half, (yl, part), e_ref) in enumerate(parts):
            t = t_ref[yl, :, half, part, :, labels].reshape(128, 256).astype(F32)
            errors = (raised[n * 128 : (n + 1) * 128] - t).astype(BF)
            e_ref[yl, :, part, :, labels] = errors.reshape(8, 16, 256)
        scores = following


def errors_of(at, step, blocks, weights, targets, before):
    return pl.pallas_call(
        functools.partial(errors_kernel, step),
        in_specs=[pl.BlockSpec(memory_space=pltpu.SMEM)] + [WHOLE] * (4 + len(before)),
        out_specs=[WHOLE] * 2,
        out_shape=[jax.ShapeDtypeStruct((2, 8, 4, 16, 1024), BF)] * 2,
        input_output_aliases={5: 0, 6: 1} if before else {},
        cost_estimate=pl.CostEstimate(
            flops=1024 * 1024 * 768, bytes_accessed=5 << 20, transcendentals=1 << 19
        ),
        compiler_params=pltpu.CompilerParams(vmem_limit_bytes=12 << 20),
        name="errors",
    )(
        at,
        *[block.reshape(2, 8, 16, 768) for block in blocks],
        weights,
        targets.reshape(2, 8, 2, 4, 16, 1024),
        *before,
    )


def turned_kernel(at_ref, w_ref, out_ref, held_ref):
    for m in range(4):
        piece = slice(m * 256, (m + 1) * 256)
        rows = w_ref[piece, :]
        held_ref[piece, :] = rows
        columns = rows.T
        for core in range(2):
            mine = jnp.where(at_ref[0] == core, 1, 0)
            for p in range(8):
                first = (2 * p + core) * 48
                out_ref[mine, p * 48 : (p + 1) * 48, piece] = columns[first : first + 48, :]


def turned(at, weights):
    return pl.pallas_call(
        turned_kernel,
        in_specs=[pl.BlockSpec(memory_space=pltpu.SMEM), WHOLE],
        out_specs=[WHOLE] * 2,
        out_shape=[
            jax.ShapeDtypeStruct((2, 384, 1024), BF),
            jax.ShapeDtypeStruct((1024, 768), BF),
        ],
        cost_estimate=pl.CostEstimate(
            flops=1024 * 1024 * 768, bytes_accessed=5 << 20, transcendentals=0
        ),
        compiler_params=pltpu.CompilerParams(vmem_limit_bytes=8 << 20),
        name="turned",
    )(at, weights)


def theirs_kernel(wt_ref, e_ref, out_ref):
    for g in range(2):
        out_ref[g] = nt(wt_ref[0], e_ref[g * 512 : (g + 1) * 512, :]).astype(BF)


def theirs_of(wt, errors):
    return pl.pallas_call(
        theirs_kernel,
        in_specs=[WHOLE] * 2,
        out_specs=WHOLE,
        out_shape=jax.ShapeDtypeStruct((2, 384, 512), BF),
        cost_estimate=pl.CostEstimate(
            flops=1024 * 1024 * 768, bytes_accessed=4 << 20, transcendentals=0
        ),
        compiler_params=pltpu.CompilerParams(vmem_limit_bytes=8 << 20),
        name="theirs",
    )(wt, errors)


def mine_kernel(wt_ref, e1_ref, e2_ref, out_ref):
    for n, e_ref in enumerate((e1_ref, e2_ref)):
        for g in range(2):
            out_ref[n, g] = nt(wt_ref[1], e_ref[g * 512 : (g + 1) * 512, :])


def mine_of(wt, errors1, errors2):
    whole = pl.BlockSpec(memory_space=VMEM)
    return pl.pallas_call(
        mine_kernel,
        in_specs=[whole] * 3,
        out_specs=whole,
        out_shape=jax.ShapeDtypeStruct((2, 2, 384, 512), F32),
        cost_estimate=pl.CostEstimate(
            flops=2 * 1024 * 1024 * 768, bytes_accessed=8 << 20, transcendentals=0
        ),
        compiler_params=pltpu.CompilerParams(vmem_limit_bytes=8 << 20),
        name="mine",
    )(wt, errors1, errors2)


def join_kernel(at_ref, m_ref, g1_ref, g2_ref, *out_refs):
    core, x, y = at_ref[0], at_ref[1], at_ref[2]
    for step, out_ref in zip((0,) + STEPS, out_refs):
        for r in range(4):
            to_x = jnp.where(core == 0, (x + step) % 4, r)
            to_y = jnp.where(core == 0, r, (y + step) % 4)
            p, yl = (to_y // 2) * 4 + to_x, to_y % 2
            for n, g_ref in enumerate((g2_ref, g1_ref)):
                out_ref[r, :, n * 512 : (n + 1) * 512] = (
                    m_ref[n, yl, p] + g_ref[yl, p].astype(F32)
                ).astype(BF)


def join(at, mine, got1, got2):
    return pl.pallas_call(
        join_kernel,
        in_specs=[pl.BlockSpec(memory_space=pltpu.SMEM)] + [WHOLE] * 3,
        out_specs=[WHOLE] * 4,
        out_shape=[jax.ShapeDtypeStruct((4, 48, 1024), BF)] * 4,
        cost_estimate=pl.CostEstimate(flops=1 << 20, bytes_accessed=6 << 20, transcendentals=0),
        compiler_params=pltpu.CompilerParams(vmem_limit_bytes=8 << 20),
        name="join",
    )(
        at,
        mine.reshape(2, 2, 8, 48, 512),
        got1.reshape(2, 8, 48, 512),
        got2.reshape(2, 8, 48, 512),
    )


def large_kernel(*refs):
    out_ref = refs[4]
    for r in range(4):
        s = refs[0][r].astype(F32)
        for ref in refs[1:4]:
            s = s + ref[r].astype(F32)
        s = s.astype(BF)
        for z in range(8):
            out_ref[r * 8 + z] = jnp.concatenate(
                [s[:, z * 64 : (z + 1) * 64], s[:, 512 + z * 64 : 512 + (z + 1) * 64]], axis=1
            )


def large_total(*blocks):
    return pl.pallas_call(
        large_kernel,
        in_specs=[WHOLE] * 4,
        out_specs=WHOLE,
        out_shape=jax.ShapeDtypeStruct((32, 48, 128), BF),
        cost_estimate=pl.CostEstimate(flops=1 << 20, bytes_accessed=2 << 20, transcendentals=0),
        compiler_params=pltpu.CompilerParams(vmem_limit_bytes=8 << 20),
        name="large_total",
    )(*blocks)


def update_kernel(e1_ref, e2_ref, f1_ref, f2_ref, w_ref, m_ref, nw_ref, nm_ref):
    dims = (((0,), (0,)), ((), ()))
    grad = lax.dot_general(e1_ref[...], f1_ref[...], dims, preferred_element_type=F32)
    grad = grad + lax.dot_general(e2_ref[...], f2_ref[...], dims, preferred_element_type=F32)
    momentum = (0.9 * m_ref[...].astype(F32) + grad).astype(BF)
    nm_ref[...] = momentum
    nw_ref[...] = (w_ref[...].astype(F32) - 0.002 * momentum.astype(F32)).astype(BF)


def update(*operands):
    labels = pl.BlockSpec((256, 768), lambda n: (n, 0))
    columns = pl.BlockSpec((1024, 256), lambda n: (0, n))
    return pl.pallas_call(
        update_kernel,
        grid=(4,),
        in_specs=[columns, columns, WHOLE, WHOLE, labels, labels],
        out_specs=[labels, labels],
        out_shape=[jax.ShapeDtypeStruct((1024, 768), BF)] * 2,
        cost_estimate=pl.CostEstimate(
            flops=4 * 1024 * 1024 * 768, bytes_accessed=12 << 20, transcendentals=0
        ),
        compiler_params=pltpu.CompilerParams(vmem_limit_bytes=24 << 20),
        name="update",
    )(*operands)


def place(core, x, y, step, n):
    from_x, from_y = (x - step) % 4, (y - step) % 4
    return (
        jnp.where(core == 0, n, from_y % 2),
        jnp.where(core == 0, from_x, (from_y // 2) * 2 + n),
    )


def by_block_kernel(at_ref, *refs):
    out_ref = refs[4]
    for step, in_ref in zip((0,) + STEPS, refs):
        for n in range(2):
            yl, part = place(at_ref[0], at_ref[1], at_ref[2], step, n)
            out_ref[yl, :, part] = in_ref[n]


def by_block(at, blocks):
    out = pl.pallas_call(
        by_block_kernel,
        in_specs=[pl.BlockSpec(memory_space=pltpu.SMEM)] + [WHOLE] * 4,
        out_specs=WHOLE,
        out_shape=jax.ShapeDtypeStruct((2, 8, 4, 16, 768), BF),
        cost_estimate=pl.CostEstimate(flops=1 << 20, bytes_accessed=3 << 20, transcendentals=0),
        compiler_params=pltpu.CompilerParams(vmem_limit_bytes=8 << 20),
        name="by_block",
    )(at, *[block.reshape(2, 8, 16, 768) for block in blocks])
    return out.reshape(1024, 768)


def program(features, weights, momentum, targets):
    ic = lax.axis_index("c")
    ix, iyh, iyl = lax.axis_index("x"), lax.axis_index("yh"), lax.axis_index("yl")
    at = jnp.stack([ic, ix, iyh * 2 + iyl]).astype(jnp.int32)
    quarter = jnp.where(ic == 0, ix, iyh * 2 + ix % 2)
    piece = lax.dynamic_slice_in_dim(features, ic * 64 + quarter * 16, 16, 0)
    other = jnp.stack([1 - ic, ix, iyh * 2 + iyl]).astype(jnp.int32)
    piece, at, other = lax.optimization_barrier((piece, at, other))
    a = exchanged(jnp.broadcast_to(piece[None], (16, 16, 768)), GATHER)
    a, weights = lax.optimization_barrier((a, weights))
    a = a.reshape(256, 768)
    blocks = [a] + [forward(a, d) for d in STEPS]
    wt, held = turned(at, weights)
    errors, others = (), []
    for step, block in zip((0,) + STEPS, blocks):
        if step == 1:
            block, errors, wt = lax.optimization_barrier((block, errors, wt))
        others.append(swapped(block))
        errors = errors_of(at, step, (block, others[-1]), held, targets, errors)
    errors1, errors2 = (e.reshape(1024, 1024) for e in errors)
    got1 = swapped(theirs_of(wt, errors1))
    got2 = swapped(theirs_of(wt, errors2))
    own, *chunks = join(at, mine_of(wt, errors1, errors2), got1, got2)
    got = [forward(chunk, d) for chunk, d in zip(chunks, STEPS)]
    rows1, rows2 = by_block(at, blocks), by_block(other, others)
    updated = update(errors1, errors2, rows1, rows2, held, momentum)
    got, updated = lax.optimization_barrier((got, updated))
    new_weights, new_momentum = updated
    u = exchanged(large_total(own, *got), SMALL)
    total = jnp.sum(u.astype(F32), 0).T.astype(BF)
    feature_grad = jnp.where(ic == 0, total, jnp.roll(total, 64, 0))
    return (new_weights, new_momentum, feature_grad)


def solution(mesh):
    fine = Mesh(mesh.devices.reshape(2, 4, 2, 2, 8), WIDE + BLK)
    both = WIDE + BLK
    return jax.shard_map(
        program,
        mesh=fine,
        in_specs=(P(BLK, None), P(both, None), P(both, None), P(None, both)),
        out_specs=(P(both, None), P(both, None), P(BLK, WIDE)),
        check_vma=False,
    )
```

```python
import functools

import jax
import jax.numpy as jnp
from jax import lax
from jax.experimental import pallas as pl
from jax.experimental.pallas import tpu as pltpu
from jax.sharding import Mesh, PartitionSpec as P


WIDE = ("yh", "x", "c")
BLK = ("yl", "z")
BF = jnp.bfloat16
F32 = jnp.float32
VMEM = pltpu.VMEM
WHOLE = pl.BlockSpec(memory_space=VMEM)


def device(yh, x, c, yl, z):
    return (((yh * 4 + x) * 2 + c) * 2 + yl) * 8 + z


def plane_device(c, along, across, z):
    x, y = (across, along) if c == 0 else (along, across)
    return device(y // 2, x, c, y % 2, z)


LARGE = [
    [plane_device(c, n, m, z) for m in range(4)]
    for c in range(2)
    for n in range(4)
    for z in range(8)
]
SMALL = [
    [plane_device(c, n, m, z) for n in range(4) for z in range(8)]
    for c in range(2)
    for m in range(4)
]


GATHER = [
    [device(yh, x, 0, yl, z) for yl in range(2) for z in range(8)]
    for yh in range(2)
    for x in range(4)
] + [
    [device(yh, 2 * pair + n, 1, yl, z) for n in range(2) for z in range(8)]
    for yh in range(2)
    for yl in range(2)
    for pair in range(2)
]


def exchanged(chunks, which):
    return lax.all_to_all(chunks, WIDE + BLK, 0, 0, axis_index_groups=which)


STEPS = (1, 3, 2)


def forward(block, step):
    route = [(g[i], g[(i + step) % 4]) for g in LARGE for i in range(4)]
    return lax.ppermute(block, WIDE + BLK, route)


def swapped(block):
    return lax.ppermute(block, "c", [(0, 1), (1, 0)])


def nt(a, b):
    return lax.dot_general(a, b, (((1,), (1,)), ((), ())), preferred_element_type=F32)


def errors_kernel(step, at_ref, f1_ref, f2_ref, w_ref, t_ref, *refs):
    core, x, y = at_ref[0], at_ref[1], at_ref[2]
    rows = jnp.concatenate([f1_ref[...].reshape(256, 768), f2_ref[...].reshape(256, 768)])
    parts = [
        (half, place(half, x, y, step, n), e_ref)
        for half, e_ref in ((core, refs[-2]), (1 - core, refs[-1]))
        for n in range(2)
    ]
    span = [slice(m * 256, (m + 1) * 256) for m in range(4)]
    scores = nt(rows, w_ref[span[0], :])
    for m, labels in enumerate(span):
        following = nt(rows, w_ref[span[m + 1], :]) if m < 3 else None
        raised = 0.5 * jnp.tanh(0.5 * scores) + 0.5
        for n, (half, (yl, part), e_ref) in enumerate(parts):
            t = t_ref[yl, :, half, part, :, labels].reshape(128, 256).astype(F32)
            errors = (raised[n * 128 : (n + 1) * 128] - t).astype(BF)
            e_ref[yl, :, part, :, labels] = errors.reshape(8, 16, 256)
        scores = following


def errors_of(at, step, blocks, weights, targets, before):
    return pl.pallas_call(
        functools.partial(errors_kernel, step),
        in_specs=[pl.BlockSpec(memory_space=pltpu.SMEM)] + [WHOLE] * (4 + len(before)),
        out_specs=[WHOLE] * 2,
        out_shape=[jax.ShapeDtypeStruct((2, 8, 4, 16, 1024), BF)] * 2,
        input_output_aliases={5: 0, 6: 1} if before else {},
        cost_estimate=pl.CostEstimate(
            flops=1024 * 1024 * 768, bytes_accessed=5 << 20, transcendentals=1 << 19
        ),
        compiler_params=pltpu.CompilerParams(vmem_limit_bytes=12 << 20),
        name="errors",
    )(
        at,
        *[block.reshape(2, 8, 16, 768) for block in blocks],
        weights,
        targets.reshape(2, 8, 2, 4, 16, 1024),
        *before,
    )


def turned_kernel(at_ref, w_ref, out_ref, held_ref):
    for m in range(4):
        piece = slice(m * 256, (m + 1) * 256)
        rows = w_ref[piece, :]
        held_ref[piece, :] = rows
        columns = rows.T
        for core in range(2):
            mine = jnp.where(at_ref[0] == core, 1, 0)
            for p in range(8):
                first = (2 * p + core) * 48
                out_ref[mine, p * 48 : (p + 1) * 48, piece] = columns[first : first + 48, :]


def turned(at, weights):
    return pl.pallas_call(
        turned_kernel,
        in_specs=[pl.BlockSpec(memory_space=pltpu.SMEM), WHOLE],
        out_specs=[WHOLE] * 2,
        out_shape=[
            jax.ShapeDtypeStruct((2, 384, 1024), BF),
            jax.ShapeDtypeStruct((1024, 768), BF),
        ],
        cost_estimate=pl.CostEstimate(
            flops=1024 * 1024 * 768, bytes_accessed=5 << 20, transcendentals=0
        ),
        compiler_params=pltpu.CompilerParams(vmem_limit_bytes=8 << 20),
        name="turned",
    )(at, weights)


def theirs_kernel(wt_ref, e_ref, out_ref):
    for g in range(2):
        out_ref[g] = nt(wt_ref[0], e_ref[g * 512 : (g + 1) * 512, :]).astype(BF)


def theirs_of(wt, errors):
    return pl.pallas_call(
        theirs_kernel,
        in_specs=[WHOLE] * 2,
        out_specs=WHOLE,
        out_shape=jax.ShapeDtypeStruct((2, 384, 512), BF),
        cost_estimate=pl.CostEstimate(
            flops=1024 * 1024 * 768, bytes_accessed=4 << 20, transcendentals=0
        ),
        compiler_params=pltpu.CompilerParams(vmem_limit_bytes=8 << 20),
        name="theirs",
    )(wt, errors)


def mine_kernel(wt_ref, e1_ref, e2_ref, out_ref):
    for n, e_ref in enumerate((e1_ref, e2_ref)):
        for g in range(2):
            out_ref[n, g] = nt(wt_ref[1], e_ref[g * 512 : (g + 1) * 512, :])


def mine_of(wt, errors1, errors2):
    whole = pl.BlockSpec(memory_space=VMEM)
    return pl.pallas_call(
        mine_kernel,
        in_specs=[whole] * 3,
        out_specs=whole,
        out_shape=jax.ShapeDtypeStruct((2, 2, 384, 512), F32),
        cost_estimate=pl.CostEstimate(
            flops=2 * 1024 * 1024 * 768, bytes_accessed=8 << 20, transcendentals=0
        ),
        compiler_params=pltpu.CompilerParams(vmem_limit_bytes=8 << 20),
        name="mine",
    )(wt, errors1, errors2)


def join_kernel(at_ref, m_ref, g1_ref, g2_ref, *out_refs):
    core, x, y = at_ref[0], at_ref[1], at_ref[2]
    for step, out_ref in zip((0,) + STEPS, out_refs):
        for r in range(4):
            to_x = jnp.where(core == 0, (x + step) % 4, r)
            to_y = jnp.where(core == 0, r, (y + step) % 4)
            p, yl = (to_y // 2) * 4 + to_x, to_y % 2
            for n, g_ref in enumerate((g2_ref, g1_ref)):
                out_ref[r, :, n * 512 : (n + 1) * 512] = (
                    m_ref[n, yl, p] + g_ref[yl, p].astype(F32)
                ).astype(BF)


def join(at, mine, got1, got2):
    return pl.pallas_call(
        join_kernel,
        in_specs=[pl.BlockSpec(memory_space=pltpu.SMEM)] + [WHOLE] * 3,
        out_specs=[WHOLE] * 4,
        out_shape=[jax.ShapeDtypeStruct((4, 48, 1024), BF)] * 4,
        cost_estimate=pl.CostEstimate(flops=1 << 20, bytes_accessed=6 << 20, transcendentals=0),
        compiler_params=pltpu.CompilerParams(vmem_limit_bytes=8 << 20),
        name="join",
    )(
        at,
        mine.reshape(2, 2, 8, 48, 512),
        got1.reshape(2, 8, 48, 512),
        got2.reshape(2, 8, 48, 512),
    )


def large_kernel(*refs):
    out_ref = refs[4]
    for r in range(4):
        s = refs[0][r].astype(F32)
        for ref in refs[1:4]:
            s = s + ref[r].astype(F32)
        s = s.astype(BF)
        for z in range(8):
            out_ref[r * 8 + z] = jnp.concatenate(
                [s[:, z * 64 : (z + 1) * 64], s[:, 512 + z * 64 : 512 + (z + 1) * 64]], axis=1
            )


def large_total(*blocks):
    return pl.pallas_call(
        large_kernel,
        in_specs=[WHOLE] * 4,
        out_specs=WHOLE,
        out_shape=jax.ShapeDtypeStruct((32, 48, 128), BF),
        cost_estimate=pl.CostEstimate(flops=1 << 20, bytes_accessed=2 << 20, transcendentals=0),
        compiler_params=pltpu.CompilerParams(vmem_limit_bytes=8 << 20),
        name="large_total",
    )(*blocks)


def small_kernel(at_ref, u_ref, out_ref):
    s = u_ref[0].astype(F32)
    for n in range(1, 32):
        s = s + u_ref[n].astype(F32)
    turned_halves = jnp.concatenate([s[:, 64:], s[:, :64]], axis=1)
    out_ref[...] = jnp.where(at_ref[0] == 0, s, turned_halves).astype(BF)


def small_total(at, u):
    return pl.pallas_call(
        small_kernel,
        in_specs=[pl.BlockSpec(memory_space=pltpu.SMEM), WHOLE],
        out_specs=WHOLE,
        out_shape=jax.ShapeDtypeStruct((48, 128), BF),
        cost_estimate=pl.CostEstimate(flops=1 << 18, bytes_accessed=1 << 19, transcendentals=0),
        compiler_params=pltpu.CompilerParams(vmem_limit_bytes=4 << 20),
        name="small_total",
    )(at, u)


def update_kernel(e1_ref, e2_ref, f1_ref, f2_ref, w_ref, m_ref, nw_ref, nm_ref):
    dims = (((0,), (0,)), ((), ()))
    grad = lax.dot_general(e1_ref[...], f1_ref[...], dims, preferred_element_type=F32)
    grad = grad + lax.dot_general(e2_ref[...], f2_ref[...], dims, preferred_element_type=F32)
    momentum = (0.9 * m_ref[...].astype(F32) + grad).astype(BF)
    nm_ref[...] = momentum
    nw_ref[...] = (w_ref[...].astype(F32) - 0.002 * momentum.astype(F32)).astype(BF)


def update(*operands):
    labels = pl.BlockSpec((256, 768), lambda n: (n, 0))
    columns = pl.BlockSpec((1024, 256), lambda n: (0, n))
    return pl.pallas_call(
        update_kernel,
        grid=(4,),
        in_specs=[columns, columns, WHOLE, WHOLE, labels, labels],
        out_specs=[labels, labels],
        out_shape=[jax.ShapeDtypeStruct((1024, 768), BF)] * 2,
        cost_estimate=pl.CostEstimate(
            flops=4 * 1024 * 1024 * 768, bytes_accessed=12 << 20, transcendentals=0
        ),
        compiler_params=pltpu.CompilerParams(vmem_limit_bytes=24 << 20),
        name="update",
    )(*operands)


def place(core, x, y, step, n):
    from_x, from_y = (x - step) % 4, (y - step) % 4
    return (
        jnp.where(core == 0, n, from_y % 2),
        jnp.where(core == 0, from_x, (from_y // 2) * 2 + n),
    )


def by_block_kernel(at_ref, *refs):
    out_ref = refs[4]
    for step, in_ref in zip((0,) + STEPS, refs):
        for n in range(2):
            yl, part = place(at_ref[0], at_ref[1], at_ref[2], step, n)
            out_ref[yl, :, part] = in_ref[n]


def by_block(at, blocks):
    out = pl.pallas_call(
        by_block_kernel,
        in_specs=[pl.BlockSpec(memory_space=pltpu.SMEM)] + [WHOLE] * 4,
        out_specs=WHOLE,
        out_shape=jax.ShapeDtypeStruct((2, 8, 4, 16, 768), BF),
        cost_estimate=pl.CostEstimate(flops=1 << 20, bytes_accessed=3 << 20, transcendentals=0),
        compiler_params=pltpu.CompilerParams(vmem_limit_bytes=8 << 20),
        name="by_block",
    )(at, *[block.reshape(2, 8, 16, 768) for block in blocks])
    return out.reshape(1024, 768)


def program(features, weights, momentum, targets):
    ic = lax.axis_index("c")
    ix, iyh, iyl = lax.axis_index("x"), lax.axis_index("yh"), lax.axis_index("yl")
    at = jnp.stack([ic, ix, iyh * 2 + iyl]).astype(jnp.int32)
    quarter = jnp.where(ic == 0, ix, iyh * 2 + ix % 2)
    piece = lax.dynamic_slice_in_dim(features, ic * 64 + quarter * 16, 16, 0)
    other = jnp.stack([1 - ic, ix, iyh * 2 + iyl]).astype(jnp.int32)
    piece, at, other = lax.optimization_barrier((piece, at, other))
    a = exchanged(jnp.broadcast_to(piece[None], (16, 16, 768)), GATHER)
    a, weights = lax.optimization_barrier((a, weights))
    a = a.reshape(256, 768)
    blocks = [a] + [forward(a, d) for d in STEPS]
    wt, held = turned(at, weights)
    errors, others = (), []
    for step, block in zip((0,) + STEPS, blocks):
        if step == 1:
            block, errors, wt = lax.optimization_barrier((block, errors, wt))
        others.append(swapped(block))
        errors = errors_of(at, step, (block, others[-1]), held, targets, errors)
    errors1, errors2 = (e.reshape(1024, 1024) for e in errors)
    got1 = swapped(theirs_of(wt, errors1))
    got2 = swapped(theirs_of(wt, errors2))
    own, *chunks = join(at, mine_of(wt, errors1, errors2), got1, got2)
    got = [forward(chunk, d) for chunk, d in zip(chunks, STEPS)]
    rows1, rows2 = by_block(at, blocks), by_block(other, others)
    updated = update(errors1, errors2, rows1, rows2, held, momentum)
    got, updated = lax.optimization_barrier((got, updated))
    new_weights, new_momentum = updated
    u = exchanged(large_total(own, *got), SMALL)
    feature_grad = small_total(at, u).T
    return (new_weights, new_momentum, feature_grad)


def solution(mesh):
    fine = Mesh(mesh.devices.reshape(2, 4, 2, 2, 8), WIDE + BLK)
    both = WIDE + BLK
    return jax.shard_map(
        program,
        mesh=fine,
        in_specs=(P(BLK, None), P(both, None), P(both, None), P(None, both)),
        out_specs=(P(both, None), P(both, None), P(BLK, WIDE)),
        check_vma=False,
    )
```
